256 devices in a mesh: seq: 16 (over z, core), tp: 16 (over y, x).
Axes of the slice: x: 4, y: 4, z: 8, core: 2. Of those that a mesh axis runs over, the one named last changes fastest.
Arguments:
- tokens: bfloat16 [4096, 4608], P('seq', 'tp'), may hold values from -6 to 6
- attention_gain: float32 [4608], replicated, may hold values from 0.25 to 1.75
- query_weight: bfloat16 [4608, 4096], P(None, 'tp'), may hold values from -0.09375 to 0.09375
- key_weight: bfloat16 [4608, 2048], P(None, 'tp'), may hold values from -0.09375 to 0.09375
- value_weight: bfloat16 [4608, 2048], P(None, 'tp'), may hold values from -0.09375 to 0.09375
- output_weight: bfloat16 [4096, 4608], P('tp'), may hold values from -0.09375 to 0.09375
- post_gain: float32 [4608], replicated, may hold values from 0.25 to 1.75
- local_gain: float32 [4608], replicated, may hold values from 0.25 to 1.75
- local_query_weight: bfloat16 [4608, 4096], P(None, 'tp'), may hold values from -0.09375 to 0.09375
- local_key_weight: bfloat16 [4608, 2048], P(None, 'tp'), may hold values from -0.09375 to 0.09375
- local_value_weight: bfloat16 [4608, 2048], P(None, 'tp'), may hold values from -0.09375 to 0.09375
Outputs:
- hidden: bfloat16 [4096, 4608], P('seq', 'tp')
- local_heads: bfloat16 [4096, 4096], P('seq', 'tp')
The draws below stay inside these ranges and needn't reach their ends.
All inputs are finite; a program needn't handle non-finite values.
Results may differ from the reference program's by a relative error of at most 0.02.
Values may be sent and summed in bfloat16 or wider, within the bound.
A program may use at most 128 MiB of HBM per device.

```python
import jax
import jax.numpy as jnp
from jax import lax

D = 4608
HEADS = 32
KV_HEADS = 16
HEAD_DIM = 128
WINDOW = 128
TOKENS = 4096


def block_scale(stream_key, dims, shards, least, largest):
    level, own = 1.0, jax.random.fold_in(stream_key, 6)
    for dim, blocks in shards:
        heights = jnp.exp(jax.random.uniform(jax.random.fold_in(own, dim), (blocks,), jnp.float32, least / len(shards), largest / len(shards)))
        level = level * jnp.repeat(heights, dims[dim] // blocks).reshape([-1 if axis == dim else 1 for axis in range(len(dims))])
    return level


def centred(rng, dims, deviation, bound, shards=(), held_as=jnp.bfloat16):
    values = jax.random.normal(rng, dims, jnp.float32) * deviation
    if len(shards) > 0:
        values = block_scale(rng, dims, shards, -0.22, 0.18) * values
    return jnp.clip(values, min=-bound, max=bound).astype(held_as)


def setup_inputs(seed: int = 0) -> dict:
    arg_keys = jax.random.split(jax.random.key(seed), 12)
    return {
        "tokens": centred(arg_keys[0], (TOKENS, D), 1.0, 6.0, ((0, 16), (1, 16))),
        "attention_gain": jnp.clip(1.0 + 0.15 * jax.random.normal(arg_keys[1], (D,), jnp.float32), 0.25, 1.75),
        "query_weight": centred(arg_keys[2], (D, HEADS * HEAD_DIM), D ** -0.5, 0.09375, ((1, 16),)),
        "key_weight": centred(arg_keys[3], (D, KV_HEADS * HEAD_DIM), D ** -0.5, 0.09375, ((1, 16),)),
        "value_weight": centred(arg_keys[4], (D, KV_HEADS * HEAD_DIM), D ** -0.5, 0.09375, ((1, 16),)),
        "output_weight": centred(arg_keys[5], (HEADS * HEAD_DIM, D), (HEADS * HEAD_DIM) ** -0.5, 0.09375, ((0, 16),)),
        "post_gain": jnp.clip(1.0 + 0.15 * jax.random.normal(arg_keys[6], (D,), jnp.float32), 0.25, 1.75),
        "local_gain": jnp.clip(1.0 + 0.15 * jax.random.normal(arg_keys[7], (D,), jnp.float32), 0.25, 1.75),
        "local_query_weight": centred(arg_keys[8], (D, HEADS * HEAD_DIM), D ** -0.5, 0.09375, ((1, 16),)),
        "local_key_weight": centred(arg_keys[9], (D, KV_HEADS * HEAD_DIM), D ** -0.5, 0.09375, ((1, 16),)),
        "local_value_weight": centred(arg_keys[10], (D, KV_HEADS * HEAD_DIM), D ** -0.5, 0.09375, ((1, 16),)),
    }


SOFT_CAP = 50.0
NORM_EPS = 1e-06

def rms_scaled(values, weights):
    widened = values.astype(jnp.float32)
    factor = lax.rsqrt(lax.optimization_barrier(jnp.mean(widened * widened, axis=-1, keepdims=True)) + NORM_EPS)
    return widened * factor * weights.astype(jnp.float32)

def rotate(vectors, places):
    head_size = vectors.shape[-1]
    halfway = head_size // 2
    exponents = jnp.arange(halfway, dtype=jnp.float32) * (2.0 / head_size)
    frequency = jnp.power(jnp.float32(10000.0), -exponents)
    angles = places.astype(jnp.float32)[:, None] * frequency[None, :]
    cosine_part = jnp.cos(angles)[:, None, :]
    sine_part = jnp.sin(angles)[:, None, :]
    first_half = vectors[..., :halfway]
    second_half = vectors[..., halfway:]
    return jnp.concatenate([first_half * cosine_part - second_half * sine_part, second_half * cosine_part + first_half * sine_part], axis=-1)

def project_heads(normed, weight_query, weight_key, weight_value, places):
    row_count = normed.shape[0]
    queries = jnp.dot(normed, weight_query, preferred_element_type=jnp.float32).reshape(row_count, -1, HEAD_DIM)
    key_heads = jnp.dot(normed, weight_key, preferred_element_type=jnp.float32).reshape(row_count, -1, HEAD_DIM)
    value_heads = jnp.dot(normed, weight_value, preferred_element_type=jnp.float32).reshape(row_count, -1, HEAD_DIM)
    return (rotate(queries, places).astype(jnp.bfloat16), rotate(key_heads, places).astype(jnp.bfloat16), value_heads.astype(jnp.bfloat16))

def attention(queries, key_heads, value_heads, window_size):
    row_count = queries.shape[0]
    groups = HEADS // KV_HEADS
    grouped = jnp.transpose(queries.reshape(row_count, KV_HEADS, groups, HEAD_DIM), (1, 0, 2, 3))
    keys_first = jnp.transpose(key_heads, (1, 0, 2))
    values_first = jnp.transpose(value_heads, (1, 0, 2))
    places = jnp.arange(row_count, dtype=jnp.int32)
    offset = places[:, None] - places[None, :]
    allowed = (offset >= 0) & (offset < window_size)
    scale = float(D // HEADS) ** (-0.5)

    def one_head(operands):
        query_block, key_block, value_block = operands
        scores = jnp.einsum('qrd,kd->rqk', query_block.astype(jnp.float32), key_block.astype(jnp.float32)) * scale
        scores = SOFT_CAP * jnp.tanh(scores / SOFT_CAP)
        weights = jnp.where(allowed[None], jnp.exp(scores), jnp.float32(0.0))
        denominator = lax.optimization_barrier(jnp.sum(weights, axis=-1))
        probs = weights.astype(jnp.bfloat16)
        numerator = jnp.einsum('rqk,kd->qrd', probs.astype(jnp.float32), value_block.astype(jnp.float32))
        return (numerator / jnp.transpose(denominator)[:, :, None]).astype(jnp.bfloat16)
    stacked = lax.map(one_head, (grouped, keys_first, values_first))
    return jnp.transpose(stacked, (1, 0, 2, 3)).reshape(row_count, HEADS * HEAD_DIM)

def reference(tokens, attention_gain, query_weight, key_weight, value_weight, output_weight, post_gain, local_gain, local_query_weight, local_key_weight, local_value_weight):
    places = jnp.arange(TOKENS, dtype=jnp.int32)
    normed = rms_scaled(tokens, attention_gain).astype(jnp.bfloat16)
    queries, key_heads, value_heads = project_heads(normed, query_weight, key_weight, value_weight, places)
    attended = attention(queries, key_heads, value_heads, TOKENS)
    projected = jnp.dot(attended, output_weight, preferred_element_type=jnp.float32)
    hidden = (tokens.astype(jnp.float32) + rms_scaled(projected, post_gain)).astype(jnp.bfloat16)
    local_normed = rms_scaled(hidden, local_gain).astype(jnp.bfloat16)
    local_queries, local_keys, local_values = project_heads(local_normed, local_query_weight, local_key_weight, local_value_weight, places)
    local_heads = attention(local_queries, local_keys, local_values, WINDOW)
    return (hidden, local_heads)
```

```python
import functools
import math

import jax
import jax.numpy as jnp
from jax import lax
from jax.experimental import pallas as pl
from jax.experimental.pallas import tpu as pltpu
from jax.sharding import PartitionSpec as P

F32 = jnp.float32
BF16 = jnp.bfloat16
MESH = pl.DeviceIdType.MESH

D = 4608
ROWS = 256
SIDE = 4
SHARE = 16
COLS = 288
WIDE = 384
HALF = D // 2
QUARTER = D // 4
HEAD = 128
WINDOW = 128
NORM_EPS = 1e-06
SOFT_CAP = 50.0
SCORE_SCALE = float(D // 32) ** (-0.5) / SOFT_CAP
EXP_SCALE = SOFT_CAP * math.log2(math.e)


def mod(a, n):
    return lax.rem(a + n, n)


class Copies:
    def __init__(self, send_sems, recv_sems):
        self.send_sems, self.recv_sems = send_sems, recv_sems
        self.started = []

    def start(self, src, dst, device, when=None):
        k = len(self.started)
        copy = pltpu.make_async_remote_copy(
            src_ref=src,
            dst_ref=dst,
            send_sem=self.send_sems.at[k],
            recv_sem=self.recv_sems.at[k],
            device_id=device,
            device_id_type=MESH,
        )
        self.started.append((copy, when))
        if when is None:
            copy.start()
        else:
            pl.when(when)(copy.start)
        return copy

    def finish(self):
        for copy, when in self.started:
            if when is None:
                copy.wait_send()
            else:
                pl.when(when)(copy.wait_send)


def part_of(d):
    return 0 if d == 1 else 1


def gather_square(copies, piece, x, y, between):
    def place(h, first, second):
        dy, dx = (second, first) if h == 0 else (first, second)
        return mod(y + dy, SIDE), mod(x + dx, SIDE)

    def send(h, axis, d, first, second, part):
        by, bx = place(h, first, second)
        ty, tx = place(h, *((d, 0) if axis == 1 else (0, d)))
        ref = piece(by, bx, h, part)
        return copies.start(ref, ref, {"tp": ty * SIDE + tx})

    both = [(h, d) for h in (0, 1) for d in (1, -1)]
    near, far, side, last = {}, {}, {}, {}
    for h, d in both:
        near[h, d] = send(h, 1, d, 0, 0, None)
    for h, d in both:
        side[h, d, 0] = send(h, 2, d, 0, 0, None)
    between(0)
    for h, d in both:
        near[h, d].wait_recv()
        far[h, d] = send(h, 1, d, -d, 0, part_of(d))
        for e in (1, -1):
            side[h, e, -d] = send(h, 2, e, -d, 0, None)
    for h, d in both:
        side[h, d, 0].wait_recv()
        last[h, d, 0] = send(h, 2, d, 0, -d, part_of(d))
    between(1)
    for h in (0, 1):
        for d in (1, -1):
            far[h, d].wait_recv()
        for e in (1, -1):
            side[h, e, 2] = send(h, 2, e, 2, 0, None)
    for o in (1, -1):
        for h, d in both:
            side[h, d, o].wait_recv()
            last[h, d, o] = send(h, 2, d, o, -d, part_of(d))
    between(2)
    for h, d in both:
        side[h, d, 2].wait_recv()
        last[h, d, 2] = send(h, 2, d, 2, -d, part_of(d))
    for o in (0, 1, -1, 2):
        for h, d in both:
            last[h, d, o].wait_recv()
    between(3)


def sum_square(copies, terms, two, one, held, two_b, one_b, x, y):
    def place(h, along, across):
        dy, dx = (along, across) if h == 0 else (across, along)
        return mod(y + dy, SIDE), mod(x + dx, SIDE)

    def device(h, axis, d):
        ty, tx = place(h, *((d, 0) if axis == 1 else (0, d)))
        return {"tp": ty * SIDE + tx}

    def term(h, along, across, part=None):
        ty, tx = place(h, along, across)
        if part is None:
            return terms.at[ty, tx, :, pl.ds(HALF * h, HALF)]
        return terms.at[ty, tx, :, pl.ds(HALF * h + QUARTER * part, QUARTER)]

    def cut(ref, part):
        return ref.at[:, pl.ds(QUARTER * part, QUARTER)]

    def add(into, other):
        into[...] = (into[...].astype(F32) + other[...].astype(F32)).astype(BF16)

    both = [(h, d) for h in (0, 1) for d in (1, -1)]
    a, b, c = {}, {}, {}

    def send_far(e):
        for h, d in both:
            p = part_of(d)
            a[h, e, d] = copies.start(term(h, 2, e, p), two.at[h, e, p], device(h, 1, d))

    def send_raw(e):
        for h, d in both:
            p = part_of(d)
            b[h, e, d] = copies.start(
                term(h, d, e, 1 - p), cut(one.at[h, e, p], 1 - p), device(h, 1, d)
            )

    def send_summed(e):
        for h, d in both:
            p = part_of(d)
            a[h, e, d].wait_recv()
            mine = term(h, d, e, p)
            add(mine, two.at[h, e, p])
            c[h, e, d] = copies.start(mine, cut(one.at[h, e, p], p), device(h, 1, d))

    def total(e):
        for h in (0, 1):
            for d in (1, -1):
                b[h, e, d].wait_recv()
                c[h, e, d].wait_recv()
            held[h, e] = (
                term(h, 0, e)[...].astype(F32)
                + one[h, e, 0].astype(F32)
                + one[h, e, 1].astype(F32)
            ).astype(BF16)

    a2, b2, c2 = {}, {}, {}
    spot = {1: 1, -1: 3}

    def raw_b(d):
        p = part_of(d)
        for h in (0, 1):
            b2[h, d] = copies.start(
                cut(held.at[h, spot[d]], 1 - p), cut(one_b.at[h, p], 1 - p), device(h, 2, d)
            )

    send_far(2)
    send_far(1)
    send_far(3)
    send_raw(2)
    send_summed(2)
    send_far(0)
    send_raw(1)
    send_summed(1)
    send_raw(3)
    send_summed(3)
    total(2)
    for h, d in both:
        p = part_of(d)
        a2[h, d] = copies.start(cut(held.at[h, 2], p), two_b.at[h, p], device(h, 2, d))
    send_raw(0)
    send_summed(0)
    total(1)
    raw_b(1)
    total(3)
    raw_b(-1)
    for h, d in both:
        p = part_of(d)
        a2[h, d].wait_recv()
        mine = cut(held.at[h, spot[d]], p)
        add(mine, two_b.at[h, p])
        c2[h, d] = copies.start(mine, cut(one_b.at[h, p], p), device(h, 2, d))
    total(0)
    for h, d in both:
        b2[h, d].wait_recv()
        c2[h, d].wait_recv()
    return jnp.concatenate(
        [
            held[h, 0].astype(F32) + one_b[h, 0].astype(F32) + one_b[h, 1].astype(F32)
            for h in (0, 1)
        ],
        axis=1,
    )


def turned(u, cosines, sines):
    return u * cosines + pltpu.roll(u, HEAD // 2, 1) * sines


def weights_of(queries, keys):
    s = lax.dot_general(queries, keys, (((1,), (1,)), ((), ())), preferred_element_type=F32)
    return jnp.exp2(jnp.tanh(s * SCORE_SCALE) * EXP_SCALE)


def kernel(
    nz, nc,
    tok, gain1, post, gain2, wq, wk, wv, wo, lq, lk, lv,
    hidden_out, heads_out,
    T, W1, W2, WO, acc, ssq, cosines, sines, Q, KV, num, den, att,
    terms, two, one, held, two_b, one_b, own, H, HS, LKV,
    send_sems, recv_sems, load_sems,
):
    t = lax.axis_index("tp")
    s = lax.axis_index("seq")
    y, x = lax.div(t, SIDE), lax.rem(t, SIDE)
    z, c = lax.div(s, nc), lax.rem(s, nc)
    ns = nz * nc

    barrier = pltpu.get_barrier_semaphore()
    peers = [
        {"tp": y * SIDE + mod(x + 1, SIDE)},
        {"tp": y * SIDE + mod(x - 1, SIDE)},
        {"tp": mod(y + 1, SIDE) * SIDE + x},
        {"tp": mod(y - 1, SIDE) * SIDE + x},
    ]
    if ns > 1:
        peers += [
            {"seq": mod(z + 1, nz) * nc + c},
            {"seq": mod(z - 1, nz) * nc + c},
            {"seq": z * nc + 1 - c},
            {"seq": mod(s - 1 + 2 * c, ns)},
        ]
    for peer in peers:
        pl.semaphore_signal(barrier, inc=1, device_id=peer, device_id_type=MESH)

    loads = []

    def load(src, dst):
        copy = pltpu.make_async_copy(src, dst, load_sems.at[len(loads)])
        copy.start()
        loads.append(copy)

    for w, at, width in ((wq, 0, 256), (wk, 256, 128), (wv, 384, 128)):
        load(w.at[:, pl.ds(0, 256), :], W1.at[:, pl.ds(0, 256), pl.ds(at, width)])
        for k in range(4):
            load(w.at[:, pl.ds(256, 32), :], W1.at[:, pl.ds(256 + 32 * k, 32), pl.ds(at, width)])
    first_loads = len(loads)
    load(wo, WO)
    load(lk, W2.at[:, pl.ds(256, 128)])
    load(lv, W2.at[:, pl.ds(384, 128)])
    load(lq, W2.at[:, pl.ds(0, 256)])

    T[y, x, 0, 0:ROWS, :] = tok[:, 0:128]
    T[y, x, 1, 0:ROWS, :] = tok[:, 128:256]
    for half in (0, 1):
        T[y, x, half, ROWS:COLS, :] = jnp.concatenate(
            [tok[32 * (4 * half + k) : 32 * (4 * half + k + 1), 256:288] for k in range(4)], axis=1
        )
    pl.semaphore_wait(barrier, len(peers))

    copies = Copies(send_sems, recv_sems)

    row = lax.broadcasted_iota(jnp.int32, (ROWS, HEAD), 0)
    lane = lax.broadcasted_iota(jnp.int32, (ROWS, HEAD), 1)
    tail_mask = lax.rem(lax.div(row, 32), 4) == lax.div(lane, 32)

    def take(by, bx):
        k = by * SIDE + bx
        tails = [T[by, bx, half, ROWS:COLS, :].astype(F32) for half in (0, 1)]
        parts = [
            T[by, bx, 0, 0:ROWS, :].astype(F32),
            T[by, bx, 1, 0:ROWS, :].astype(F32),
            jnp.where(tail_mask, jnp.concatenate([tails[0]] * 4 + [tails[1]] * 4, axis=0), 0.0),
        ]
        ssq[...] += sum(u * u for u in parts)
        gain = gain1[pl.ds(k, 1), :]
        scaled = jnp.concatenate(
            [(u * gain[:, HEAD * i : HEAD * (i + 1)]).astype(BF16) for i, u in enumerate(parts)],
            axis=1,
        )
        acc[...] += jnp.dot(scaled, W1[k], preferred_element_type=F32)

    def take_offset(dy, dx):
        take(mod(y + dy, SIDE), mod(x + dx, SIDE))

    def over(count, body):
        def step(i, carry):
            body(i)
            return carry

        lax.fori_loop(0, count, step, 0)

    def between_first(stage):
        if stage == 0:
            half_lane = jnp.where(lane < HEAD // 2, lane, lane - HEAD // 2)
            frequency = jnp.exp(half_lane.astype(F32) * (-math.log(10000.0) / (HEAD // 2)))
            angle = (row + s * ROWS).astype(F32) * frequency
            cosines[...] = jnp.cos(angle)
            sine = jnp.sin(angle)
            sines[...] = jnp.where(lane < HEAD // 2, -sine, sine)
            acc[...] = jnp.zeros_like(acc)
            ssq[...] = jnp.zeros_like(ssq)
            num[...] = jnp.zeros_like(num)
            den[...] = jnp.zeros_like(den)
        elif stage == 1:
            for copy in loads[:first_loads]:
                copy.wait()
            take_offset(0, 0)

            def near(i):
                step, alongside = 1 + 2 * lax.rem(i, 2), lax.div(i, 2)
                take_offset(step * alongside, step * (1 - alongside))

            over(4, near)
        elif stage == 2:
            over(4, lambda i: take_offset(1 + 2 * lax.rem(i, 2), 1 + 2 * lax.div(i, 2)))
        elif stage == 3:
            over(4, lambda i: take_offset(2, i))
            over(3, lambda i: take_offset(i + lax.div(i, 2), 2))

    def block(by, bx, h, part):
        if part is None:
            return T.at[by, bx, h]
        return T.at[by, bx, h, pl.ds(144 * part, 144), :]

    gather_square(copies, block, x, y, between_first)

    def scale_of(squares):
        return lax.rsqrt(jnp.sum(squares, axis=1, keepdims=True) * (1.0 / D) + NORM_EPS)

    factor = scale_of(ssq[...])
    ring = {}

    def send_along(dirn, hop, kv):
        zb = mod(z - dirn * (hop - 1), nz)
        ref = KV.at[zb, c, kv]
        ring[dirn, hop, kv] = copies.start(ref, ref, {"seq": mod(z + dirn, nz) * nc + c})

    def send_across(dirn, hop, kv):
        ref = KV.at[mod(z - dirn * hop, nz), c, kv]
        ring["across", dirn, hop, kv] = copies.start(ref, ref, {"seq": z * nc + 1 - c})

    def allowed(dirn, hop, kv):
        return hop <= 3 or (hop == 4 and (dirn == 1) == (kv == 0))

    KV[z, c, 0] = turned(acc[:, 256:384] * factor, cosines[...], sines[...]).astype(BF16)
    if ns > 1:
        for dirn in (1, -1):
            send_along(dirn, 1, 0)
    KV[z, c, 1] = (acc[:, 384:512] * factor).astype(BF16)
    if ns > 1:
        for dirn in (1, -1):
            send_along(dirn, 1, 1)
        for kv in (0, 1):
            send_across(1, 0, kv)
    for h in (0, 1):
        Q[ROWS * h : ROWS * (h + 1), :] = turned(
            acc[:, HEAD * h : HEAD * (h + 1)] * factor, cosines[...], sines[...]
        ).astype(BF16)

    def attend(zb, cb, causal):
        for i in range(4):
            at = pl.ds(128 * i, 128)
            w = weights_of(Q[at, :], KV[zb, cb, 0])
            if causal:
                r = lax.broadcasted_iota(jnp.int32, w.shape, 0) + 128 * (i % 2)
                w = jnp.where(lax.broadcasted_iota(jnp.int32, w.shape, 1) <= r, w, 0.0)
            den[at, :] += w[:, 0:128] + w[:, 128:256]
            num[at, :] += jnp.dot(w.astype(BF16), KV[zb, cb, 1], preferred_element_type=F32)

    def attend_if(zb, cb):
        @pl.when(zb * nc + cb < s)
        def _():
            attend(zb, cb, False)

    attend(z, c, True)

    own[...] = jnp.zeros_like(own)
    tail_lane = lax.broadcasted_iota(jnp.int32, (SHARE, HEAD), 1)
    for k in range(16):
        by, bx = divmod(k, SIDE)
        rows = pl.ds(pl.multiple_of(t * SHARE, SHARE), SHARE)
        tail_rows = pl.ds(pl.multiple_of(ROWS + SHARE * lax.rem(t, 2), SHARE), SHARE)
        tail = T[by, bx, lax.div(t, 8), tail_rows, :].astype(F32)
        tail = pltpu.roll(tail, lax.rem(HEAD - 32 * lax.rem(lax.div(t, 2), 4), HEAD), 1)
        joined = jnp.concatenate(
            [
                T[by, bx, 0, rows, :].astype(F32),
                T[by, bx, 1, rows, :].astype(F32),
                jnp.where(tail_lane < 32, tail, 0.0),
            ],
            axis=1,
        )
        start = 128 * (2 * k + k // 4)
        if k % 4:
            joined = pltpu.roll(joined, 32 * (k % 4), 1)
        own[:, start : start + WIDE] += joined

    if ns > 1:
        def across(dirn, hop):
            for kv in (0, 1):
                if allowed(dirn, hop, kv):
                    ring["across", dirn, hop, kv].wait_recv()

        for hop in (1, 2, 3, 4):
            for kv in (0, 1):
                for dirn in (1, -1):
                    if allowed(dirn, hop, kv):
                        ring[dirn, hop, kv].wait_recv()
                        if allowed(dirn, hop + 1, kv):
                            send_along(dirn, hop + 1, kv)
                        send_across(dirn, hop, kv)
            if hop < 4:
                over(2, lambda i, hop=hop: attend_if(mod(z - hop + 2 * hop * i, nz), c))
            else:
                attend_if(mod(z - 4, nz), c)
            if hop == 1:
                across(1, 0)
                attend_if(z, 1 - c)
            else:
                across(1, hop - 1)
                across(-1, hop - 1)
                over(2, lambda i, hop=hop: attend_if(mod(z - (hop - 1) + 2 * (hop - 1) * i, nz), 1 - c))
        across(1, 4)
        across(-1, 4)
        attend_if(mod(z - 4, nz), 1 - c)

    for h in (0, 1):
        at = pl.ds(ROWS * h, ROWS)
        att[:, HEAD * h : HEAD * (h + 1)] = (
            num[at, :] / jnp.sum(den[at, :], axis=1, keepdims=True)
        ).astype(BF16)

    for copy in loads[first_loads:]:
        copy.wait()
    for n in range(D // 512):
        product = jnp.dot(att[...], WO[:, 512 * n : 512 * (n + 1)], preferred_element_type=F32)
        terms[:, :, :, 512 * n : 512 * (n + 1)] = product.astype(BF16).reshape(SIDE, SIDE, SHARE, 512)
    summed = sum_square(copies, terms, two, one, held, two_b, one_b, x, y)
    level = lax.rsqrt(jnp.sum(summed * summed, axis=1, keepdims=True) * (1.0 / D) + NORM_EPS)
    H[y, x] = (own[...] + summed * level * post[...]).astype(BF16)

    ssq[...] = jnp.zeros_like(ssq)

    def scaled_rows(by, bx):
        k = by * SIDE + bx
        rows = H[by, bx].astype(F32)
        HS[k] = (rows * gain2[...]).astype(BF16)
        squares = rows * rows
        ssq[pl.ds(pl.multiple_of(k * SHARE, SHARE), SHARE), :] = sum(
            squares[:, HEAD * i : HEAD * (i + 1)] for i in range(D // HEAD)
        )

    def between_second(stage):
        def at(dy, dx):
            scaled_rows(mod(y + dy, SIDE), mod(x + dx, SIDE))

        if stage == 1:
            at(0, 0)

            def near(i):
                step, alongside = 1 + 2 * lax.rem(i, 2), lax.div(i, 2)
                at(step * alongside, step * (1 - alongside))

            over(4, near)
        elif stage == 2:
            over(4, lambda i: at(1 + 2 * lax.rem(i, 2), 1 + 2 * lax.div(i, 2)))
        elif stage == 3:
            over(4, lambda i: at(2, i))
            over(3, lambda i: at(i + lax.div(i, 2), 2))

    def hidden_block(by, bx, h, part):
        if part is None:
            return H.at[by, bx, :, pl.ds(HALF * h, HALF)]
        return H.at[by, bx, :, pl.ds(HALF * h + QUARTER * part, QUARTER)]

    gather_square(copies, hidden_block, x, y, between_second)

    factor = scale_of(ssq[...])
    rows = HS[...].reshape(ROWS, D)
    pair = jnp.dot(rows, W2[:, 256:512], preferred_element_type=F32) * factor
    LKV[0, WINDOW : WINDOW + ROWS, :] = turned(pair[:, 0:128], cosines[...], sines[...]).astype(BF16)
    LKV[1, WINDOW : WINDOW + ROWS, :] = pair[:, 128:256].astype(BF16)
    handed = []
    if ns > 1:
        for kv in (0, 1):
            handed.append(
                copies.start(
                    LKV.at[kv, pl.ds(ROWS, WINDOW), :],
                    LKV.at[kv, pl.ds(0, WINDOW), :],
                    {"seq": mod(s + 1, ns)},
                    when=s < ns - 1,
                )
            )

    @pl.when(s == 0)
    def _():
        LKV[:, 0:WINDOW, :] = jnp.zeros((2, WINDOW, HEAD), BF16)

    local_q = jnp.dot(rows, W2[:, 0:256], preferred_element_type=F32) * factor
    for h in (0, 1):
        Q[ROWS * h : ROWS * (h + 1), :] = turned(
            local_q[:, HEAD * h : HEAD * (h + 1)], cosines[...], sines[...]
        ).astype(BF16)

    base = pl.multiple_of(128 * (2 * t + lax.div(t, 4)), 128)
    window = H[:, :, :, pl.ds(base, WIDE)].reshape(ROWS, WIDE).astype(F32)
    window = pltpu.roll(window, lax.rem(WIDE - 32 * lax.rem(t, 4), WIDE), 1)
    hidden_out[...] = window[:, 0:COLS].astype(BF16)

    def attend_window(b):
        for h in (0, 1):
            at = pl.ds(ROWS * h + WINDOW * b, WINDOW)
            span = pl.ds(WINDOW * b, 2 * WINDOW)
            w = weights_of(Q[at, :], LKV[0, span, :])
            r = lax.broadcasted_iota(jnp.int32, w.shape, 0)
            k = lax.broadcasted_iota(jnp.int32, w.shape, 1)
            mask = (k > r) & (k <= r + WINDOW)
            if b == 0:
                mask = mask & ((k >= WINDOW) | (s > 0))
            w = jnp.where(mask, w, 0.0)
            below = jnp.sum(w, axis=1, keepdims=True)
            above = jnp.dot(w.astype(BF16), LKV[1, span, :], preferred_element_type=F32)
            heads_out[WINDOW * b : WINDOW * (b + 1), HEAD * h : HEAD * (h + 1)] = (
                above / below
            ).astype(BF16)

    attend_window(1)
    for copy in handed:
        pl.when(s > 0)(copy.wait_recv)
    attend_window(0)
    copies.finish()


COPIES = 176


def local(
    nz, nc,
    tokens, attention_gain, query_weight, key_weight, value_weight, output_weight,
    post_gain, local_gain, local_query_weight, local_key_weight, local_value_weight,
):
    blocks = attention_gain.reshape(16, COLS)
    gain1 = jnp.concatenate([blocks[:, :256]] + [blocks[:, 256:]] * 4, axis=1)
    vmem = pl.BlockSpec(memory_space=pltpu.VMEM)
    hbm = pl.BlockSpec(memory_space=pl.ANY)
    ns = nz * nc
    return pl.pallas_call(
        functools.partial(kernel, nz, nc),
        out_shape=(
            jax.ShapeDtypeStruct((ROWS, COLS), BF16),
            jax.ShapeDtypeStruct((ROWS, 256), BF16),
        ),
        in_specs=[vmem] * 4 + [hbm] * 7,
        out_specs=(vmem, vmem),
        scratch_shapes=[
            pltpu.VMEM((SIDE, SIDE, 2, COLS, 128), BF16),
            pltpu.VMEM((16, WIDE, 512), BF16),
            pltpu.VMEM((D, 512), BF16),
            pltpu.VMEM((256, D), BF16),
            pltpu.VMEM((ROWS, 512), F32),
            pltpu.VMEM((ROWS, HEAD), F32),
            pltpu.VMEM((ROWS, HEAD), F32),
            pltpu.VMEM((ROWS, HEAD), F32),
            pltpu.VMEM((2 * ROWS, HEAD), BF16),
            pltpu.VMEM((nz, nc, 2, ROWS, HEAD), BF16),
            pltpu.VMEM((2 * ROWS, HEAD), F32),
            pltpu.VMEM((2 * ROWS, HEAD), F32),
            pltpu.VMEM((ROWS, 256), BF16),
            pltpu.VMEM((SIDE, SIDE, SHARE, D), BF16),
            pltpu.VMEM((2, 4, 2, SHARE, QUARTER), BF16),
            pltpu.VMEM((2, 4, 2, SHARE, HALF), BF16),
            pltpu.VMEM((2, 4, SHARE, HALF), BF16),
            pltpu.VMEM((2, 2, SHARE, QUARTER), BF16),
            pltpu.VMEM((2, 2, SHARE, HALF), BF16),
            pltpu.VMEM((SHARE, D), F32),
            pltpu.VMEM((SIDE, SIDE, SHARE, D), BF16),
            pltpu.VMEM((16, SHARE, D), BF16),
            pltpu.VMEM((2, WINDOW + ROWS, HEAD), BF16),
            pltpu.SemaphoreType.DMA((COPIES,)),
            pltpu.SemaphoreType.DMA((COPIES,)),
            pltpu.SemaphoreType.DMA((24,)),
        ],
        compiler_params=pltpu.CompilerParams(
            collective_id=0, has_side_effects=True, vmem_limit_bytes=56 * 1024 * 1024
        ),
    )(
        tokens, gain1, post_gain.reshape(1, D), local_gain.reshape(1, D),
        query_weight.reshape(16, COLS, -1), key_weight.reshape(16, COLS, -1),
        value_weight.reshape(16, COLS, -1), output_weight,
        local_query_weight, local_key_weight, local_value_weight,
    )


def solution(mesh):
    in_specs = (
        P("seq", "tp"),
        P(),
        P(None, "tp"),
        P(None, "tp"),
        P(None, "tp"),
        P("tp", None),
        P(),
        P(),
        P(None, "tp"),
        P(None, "tp"),
        P(None, "tp"),
    )
    out_specs = (P("seq", "tp"), P("seq", "tp"))
    ns = mesh.shape["seq"]
    nc = 2 if ns > 1 else 1
    return jax.shard_map(
        functools.partial(local, ns // nc, nc),
        mesh=mesh,
        in_specs=in_specs,
        out_specs=out_specs,
        check_vma=False,
    )
```
